32 devices in a mesh: layer: 4 (over z), row: 2 (over core), col: 4 (over y, x).
Axes of the slice: x: 2, y: 2, z: 4, core: 2. Of those that a mesh axis runs over, the one named last changes fastest.
Arguments:
- panels: float32 [4096, 8192], P('row', ('layer', 'col')), may hold values from -0.0625 to 0.0625
- eigvecs: float32 [8192, 2048], P(('layer', 'row'), 'col'), may hold values from -6 to 6
Outputs:
- result: float32 [4096, 2048], P('row', 'col')
The draws below stay inside these ranges and needn't reach their ends.
All inputs are finite; a program needn't handle non-finite values.
Results may differ from the reference program's by a relative error of at most 0.0001.
Values sent between devices are 32-bit elements; how exact they have to be, the bound alone decides.
No kernel may reach another device: no remote copies, remote signals or barrier semaphores. Data moves between devices by JAX's collectives and lax.ppermute only.
A program may use at most 64 MiB of HBM per device.

```python
import jax
import jax.numpy as jnp
from jax import lax

NB = 1024
PANELS = 2
NEV = 2048
ROWS = 4096
INNER = 8192
N_LAYER = 4


def block_scale(stream_key, dims, shards, least, largest):
    loudness, own = 1.0, jax.random.fold_in(stream_key, 6)
    for axis_at, blocks in shards:
        draws = jnp.exp(jax.random.uniform(jax.random.fold_in(own, axis_at), (blocks,), jnp.float32, least / len(shards), largest / len(shards)))
        loudness = loudness * jnp.repeat(draws, dims[axis_at] // blocks).reshape([-1 if axis == axis_at else 1 for axis in range(len(dims))])
    return loudness


def bell_draw(own_key, dims, deviation, bound, pieces=(), dtype=jnp.bfloat16):
    level = block_scale(own_key, dims, pieces, -0.22, 0.18) if pieces else 1.0
    entries = jax.random.normal(own_key, dims, jnp.float32) * deviation * level
    return jnp.minimum(jnp.maximum(entries, -bound), bound).astype(dtype)


def setup_inputs(seed: int = 0) -> dict:
    arg_keys = jax.random.split(jax.random.key(seed), 3)
    return {
        "panels": bell_draw(arg_keys[0], (ROWS, INNER), INNER ** -0.5, 0.0625, ((0, 2), (1, 16)), jnp.float32),
        "eigvecs": bell_draw(arg_keys[1], (INNER, NEV), 1.0, 6.0, ((0, 8), (1, 4)), jnp.float32),
    }


def reference(panels, eigvecs):
    group = PANELS * NB
    result = jnp.zeros((panels.shape[0], eigvecs.shape[1]), jnp.float32)
    for index in range(N_LAYER):
        partial_value = jnp.dot(panels[:, index * group:(index + 1) * group], eigvecs[index * group:(index + 1) * group, :], preferred_element_type=jnp.float32, precision=lax.Precision.HIGHEST)
        result = result + partial_value
    return result
```

```python
import jax
import jax.numpy as jnp
from jax import lax
from jax.experimental import pallas as pl
from jax.experimental.pallas import tpu as pltpu
from jax.sharding import PartitionSpec as P


SHARES = (7, 6, 6, 7, 6, 6, 7, 6, 6, 7)
LAG = 3
VMEM = 12 * 2**20


def side(count):
    return max(i for i in range(1, count + 1) if i * i <= count and count % i == 0)


def halves(value):
    high = value.astype(jnp.bfloat16)
    return high, (value - high.astype(jnp.float32)).astype(jnp.bfloat16)


def pick(index, values):
    chosen = values[0]
    for i, value in enumerate(values[1:], 1):
        chosen = jnp.where(index == i, value, chosen)
    return chosen


def product_kernel(pieces, nx, sets, groups, *refs):
    parts, factors = refs[:pieces * nx], refs[pieces * nx:pieces * nx + 2 * nx * sets * groups]
    outs = refs[len(parts) + len(factors):]
    terms = [halves(part[...]) for part in parts]
    for f in range(sets):
        for g in range(groups):
            chosen = factors[2 * nx * (f * groups + g):]
            totals = [None] * pieces
            for s in range(nx):
                high, low = chosen[2 * s][...], chosen[2 * s + 1][...]
                for which, b in ((1, high), (0, low), (0, high)):
                    for i in range(pieces):
                        term = jnp.dot(terms[i * nx + s][which], b, preferred_element_type=jnp.float32)
                        totals[i] = term if totals[i] is None else totals[i] + term
            for i in range(pieces):
                out = outs[f * pieces + i]
                width = out.shape[1] // groups
                out[:, g * width:(g + 1) * width] = totals[i]


def product(pieces, sets):
    nx, groups = len(pieces[0]), len(sets[0])
    width = sets[0][0][0].shape[1] * groups
    whole = lambda value: pl.BlockSpec(value.shape, lambda i: (0, 0))
    flat = [part for piece in pieces for part in piece] + [term for each in sets for group in each for term in group]
    results = [jax.ShapeDtypeStruct((piece[0].shape[0], width), jnp.float32) for _ in sets for piece in pieces]
    flops = sum(6 * part.size * width * len(sets) for piece in pieces for part in piece)
    found = pl.pallas_call(
        lambda *refs: product_kernel(len(pieces), nx, len(sets), groups, *refs),
        grid=(1,),
        out_shape=results,
        in_specs=[whole(value) for value in flat],
        out_specs=[whole(result) for result in results],
        compiler_params=pltpu.CompilerParams(vmem_limit_bytes=VMEM),
        cost_estimate=pl.CostEstimate(flops=flops, bytes_accessed=flops // 3072, transcendentals=0),
        name="product",
    )(*flat)
    return [found[f * len(pieces):(f + 1) * len(pieces)] for f in range(len(sets))]


def solution(mesh):
    layers, rows, cols = (mesh.shape[a] for a in ("layer", "row", "col"))
    nx = side(cols)
    ny = cols // nx
    if rows % ny or layers != 4:
        raise ValueError("mesh")
    q = rows // ny

    def along_x(shift):
        return [(y * nx + x, y * nx + (x + shift) % nx) for y in range(ny) for x in range(nx)]

    def along_y(shift):
        return [(y * nx + x, (y + shift) % ny * nx + x) for y in range(ny) for x in range(nx)]

    turn = [
        ((r * ny + y) * nx + x, ((y * q + r % q) * ny + r // q) * nx + x)
        for r in range(rows) for y in range(ny) for x in range(nx) if r // q != y
    ]
    pairs = [(0, 1), (1, 0), (2, 3), (3, 2)]
    across = [(1, 2), (2, 1)]

    def add(a, b):
        return a + b

    def body(panels, eigvecs):
        layer, row = lax.axis_index("layer"), lax.axis_index("row")
        col = lax.axis_index("col")
        y, x = col // nx, col % nx
        end = (layer == 0) | (layer == layers - 1)
        depth = panels.shape[1]
        width = eigvecs.shape[1]
        groups = 2 if width % 256 == 0 else 1
        unit = panels.shape[0] // sum(SHARES)
        n = len(SHARES)
        pieces, at = [], 0
        for share in SHARES:
            pieces.append(panels[at:at + share * unit])
            at += share * unit

        own = [eigvecs[:, g * width // groups:(g + 1) * width // groups] for g in range(groups)]
        own = [lax.optimization_barrier(part) for part in own]
        stays = row // q == y
        turned = [lax.ppermute(own[g], ("row", "col"), turn) for g in range(groups)]
        gathered = {}

        def gather(i):
            gathered[i] = [lax.ppermute(pieces[i], "col", along_x(s)) for s in range(1, nx)]

        for i in range(n):
            gather(i)

        def arrange(blocks):
            count = eigvecs.shape[0] // depth
            chunks = [[block[c * depth:(c + 1) * depth] for c in range(count)] for block in blocks]
            by_y = []
            for t in range(ny):
                terms = []
                for s in range(nx):
                    k, found = (x - s) % nx, []
                    for m in range(q):
                        back = (row - (y + t) % ny * q - m) % rows
                        found += [pick(back, [chunk[c] for chunk in chunks]) for c in range(count)]
                    value = pick(k, found)
                    high = lax.reduce_precision(value, 8, 7)
                    terms += [high.astype(jnp.bfloat16), (value - high).astype(jnp.bfloat16)]
                by_y.append(terms)
            return by_y

        factors = []
        parts = [[piece] + gathered[i] for i, piece in enumerate(pieces)]
        first = [[] for _ in range(1, ny)]
        for g in range(groups):
            held = jnp.where(stays, own[g], turned[g])
            blocks = [held] + [
                lax.ppermute(held, "row", [(r, (r + s) % rows) for r in range(rows)]) for s in range(1, rows)
            ]
            factors.append(arrange(blocks))
            for t in range(1, ny):
                value = product([parts[0]], [[factors[g][t]]])[0][0]
                first[t - 1].append(lax.ppermute(value, "col", along_y(t)))
        near = [product([parts[0]], [[group[0] for group in factors]])[0][0]]
        sent = [[jnp.concatenate(pair, axis=1) for pair in first]]
        starts = [unit * sum(SHARES[:i]) for i in range(n)]
        result = jnp.zeros((panels.shape[0], width), jnp.float32)
        total, summed, done, paired, crossed = {}, {}, {}, {}, {}
        for i in range(n + LAG + 2):
            if i % 2 == 0 and i + 1 < n:
                both = parts[i + 1:i + 3]
                found = product(both, [[group[t] for group in factors] for t in range(ny)])
                near += found[0]
                for k in range(len(both)):
                    sent.append([lax.ppermute(found[t][k], "col", along_y(t)) for t in range(1, ny)])
            if i < n:
                total[i] = near[i]
                for part in sent[i]:
                    total[i] = add(total[i], part)
            if LAG <= i < n + LAG:
                done[i - LAG] = add(summed[i - LAG], crossed[i - LAG])
            if i < n + LAG:
                if i < LAG:
                    give = total[i]
                elif i >= n:
                    give = done[i - LAG]
                else:
                    give = jnp.where(end, total[i], done[i - LAG])
                paired[i] = lax.ppermute(give, "layer", pairs)
            k = i - 1
            if 0 <= k < n:
                summed[k] = add(total[k], paired[k])
                crossed[k] = lax.ppermute(summed[k], "layer", across)
            k = i - LAG - 1
            if 0 <= k < n:
                value = jnp.where(end, paired[k + LAG], done[k])
                result = lax.dynamic_update_slice(result, value, (starts[k], 0))
        return result

    in_specs = (P("row", ("layer", "col")), P(("layer", "row"), "col"))
    out_specs = P("row", "col")
    step = jax.shard_map(body, mesh=mesh, in_specs=in_specs, out_specs=out_specs, check_vma=False)

    def traced(panels, eigvecs):
        jax.eval_shape(step, panels, eigvecs)
        return step(panels, eigvecs)

    return traced
```

```python
import jax
import jax.numpy as jnp
from jax import lax
from jax.experimental import pallas as pl
from jax.experimental.pallas import tpu as pltpu
from jax.sharding import PartitionSpec as P


SHARES = (7, 6, 6, 7, 6, 6, 7, 6, 6, 7)
LAG = 3
EARLY = 5
LATE = {0: (5, 6), 1: (7,), 2: (8, 9, 10)}
WORK = {-2: (1,), -1: (2,), 1: (3,), 3: (4, 5), 5: (6, 7), 7: (8, 9), 8: (10,)}
VMEM = 12 * 2**20


def side(count):
    return max(i for i in range(1, count + 1) if i * i <= count and count % i == 0)


def halves(value):
    high = value.astype(jnp.bfloat16)
    return high, (value - high.astype(jnp.float32)).astype(jnp.bfloat16)


def product_kernel(pieces, nx, sets, groups, *refs):
    parts, factors = refs[:pieces * nx], refs[pieces * nx:pieces * nx + 2 * nx * sets * groups]
    outs = refs[len(parts) + len(factors):]
    terms = [halves(part[...]) for part in parts]
    for f in range(sets):
        for g in range(groups):
            chosen = factors[2 * nx * (f * groups + g):]
            totals = [None] * pieces
            for s in range(nx):
                high, low = chosen[2 * s][...], chosen[2 * s + 1][...]
                for which, b in ((1, high), (0, low), (0, high)):
                    for i in range(pieces):
                        term = jnp.dot(terms[i * nx + s][which], b, preferred_element_type=jnp.float32)
                        totals[i] = term if totals[i] is None else totals[i] + term
            for i in range(pieces):
                out = outs[f * pieces + i]
                width = out.shape[1] // groups
                out[:, g * width:(g + 1) * width] = totals[i]


def product(pieces, sets):
    nx, groups = len(pieces[0]), len(sets[0])
    width = sets[0][0][0].shape[1] * groups
    whole = lambda value: pl.BlockSpec(value.shape, lambda i: (0, 0))
    flat = [part for piece in pieces for part in piece] + [term for each in sets for group in each for term in group]
    results = [pltpu.VMEM((piece[0].shape[0], width), jnp.float32) for _ in sets for piece in pieces]
    flops = sum(6 * part.size * width * len(sets) for piece in pieces for part in piece)
    found = pl.pallas_call(
        lambda *refs: product_kernel(len(pieces), nx, len(sets), groups, *refs),
        grid=(1,),
        out_shape=results,
        in_specs=[whole(value) for value in flat],
        out_specs=[whole(result) for result in results],
        compiler_params=pltpu.CompilerParams(vmem_limit_bytes=VMEM),
        cost_estimate=pl.CostEstimate(flops=flops, bytes_accessed=flops // 3072, transcendentals=0),
        name="product",
    )(*flat)
    return [found[f * len(pieces):(f + 1) * len(pieces)] for f in range(len(sets))]


def arrange_kernel(nx, ny, depth, place, *refs):
    row, y, x = place[0], place[1], place[2]
    rows = len(refs) - 2 * nx * ny
    q = rows // ny
    for t in range(ny):
        for s in range(nx):
            value = None
            for back in range(rows):
                count = refs[back].shape[0] // depth
                index = (row - back + rows) % rows
                for c in range(count):
                    here = (index // q == (y + t) % ny) & ((index % q) * count + c == (x - s + nx) % nx)
                    chunk = refs[back][c * depth:(c + 1) * depth, :]
                    value = chunk if value is None else jnp.where(here, chunk, value)
            at = rows + 2 * (t * nx + s)
            refs[at][...], refs[at + 1][...] = halves(value)


def arrange(place, blocks, nx, ny, depth):
    width = blocks[0].shape[1]
    whole = lambda value: pl.BlockSpec(value.shape, lambda i: (0, 0))
    results = [pltpu.VMEM((depth, width), jnp.bfloat16)] * (2 * nx * ny)
    found = pl.pallas_call(
        lambda *refs: arrange_kernel(nx, ny, depth, *refs),
        grid=(1,),
        out_shape=results,
        in_specs=[pl.BlockSpec(memory_space=pltpu.SMEM)] + [whole(block) for block in blocks],
        out_specs=[whole(result) for result in results],
        compiler_params=pltpu.CompilerParams(vmem_limit_bytes=VMEM),
        cost_estimate=pl.CostEstimate(flops=blocks[0].size * 64, bytes_accessed=blocks[0].size * 16, transcendentals=0),
        name="arrange",
    )(place, *blocks)
    return [found[2 * nx * t:2 * nx * (t + 1)] for t in range(ny)]


def combine_kernel(counts, flag, *refs):
    ins, outs = refs[:sum(counts)], refs[sum(counts):]
    found, at = [], 0
    for count in counts:
        total = ins[at][...]
        for ref in ins[at + 1:at + count]:
            total = total + ref[...]
        found.append(total)
        at += count
    for total, out in zip(found, outs):
        out[...] = total
    if len(counts) > 1:
        outs[-1][...] = jnp.where(flag[0] == 1, found[0], found[1])


def combine(flag, *lists):
    shape = lists[0][0].shape
    flat = [value for values in lists for value in values]
    whole = pl.BlockSpec(shape, lambda i: (0, 0))
    results = [pltpu.VMEM(shape, jnp.float32)] * (len(lists) + (len(lists) > 1))
    return pl.pallas_call(
        lambda *refs: combine_kernel([len(values) for values in lists], *refs),
        grid=(1,),
        out_shape=results,
        in_specs=[pl.BlockSpec(memory_space=pltpu.SMEM)] + [whole] * len(flat),
        out_specs=[whole] * len(results),
        compiler_params=pltpu.CompilerParams(vmem_limit_bytes=VMEM),
        cost_estimate=pl.CostEstimate(flops=flat[0].size * 64, bytes_accessed=flat[0].size * 16, transcendentals=0),
        name="combine",
    )(flag, *flat)


def solution(mesh):
    layers, rows, cols = (mesh.shape[a] for a in ("layer", "row", "col"))
    nx = side(cols)
    ny = cols // nx
    if rows % ny or layers != 4:
        raise ValueError("mesh")
    q = rows // ny

    def along_x(shift):
        return [(y * nx + x, y * nx + (x + shift) % nx) for y in range(ny) for x in range(nx)]

    def along_y(shift):
        return [(y * nx + x, (y + shift) % ny * nx + x) for y in range(ny) for x in range(nx)]

    turn = [
        ((r * ny + y) * nx + x, ((y * q + r % q) * ny + r // q) * nx + x)
        for r in range(rows) for y in range(ny) for x in range(nx) if r // q != y
    ]
    pairs = [(0, 1), (1, 0), (2, 3), (3, 2)]
    across = [(1, 2), (2, 1)]

    def body(panels, eigvecs):
        layer, row = lax.axis_index("layer"), lax.axis_index("row")
        col = lax.axis_index("col")
        y, x = col // nx, col % nx
        end = (layer == 0) | (layer == layers - 1)
        depth = panels.shape[1]
        width = eigvecs.shape[1]
        groups = 2 if width % 256 == 0 else 1
        unit = panels.shape[0] // sum(SHARES)
        n = len(SHARES)
        pieces, at = [], 0
        for share in SHARES:
            pieces.append(panels[at:at + share * unit])
            at += share * unit

        own, source = [], eigvecs
        for g in range(groups):
            own.append(lax.optimization_barrier(source[:, g * width // groups:(g + 1) * width // groups]))
            if g + 1 < groups:
                source, own[g] = lax.optimization_barrier((source, own[g]))
        stays = row // q == y
        turned = [lax.ppermute(own[g], ("row", "col"), turn) for g in range(groups)]
        gathered = {}
        flag = end.astype(jnp.int32).reshape(1)

        def gather(i):
            gathered[i] = [lax.ppermute(pieces[i], "col", along_x(s)) for s in range(1, nx)]

        for i in range(EARLY):
            gather(i)

        place = jnp.stack([row, y, x])
        factors = []
        parts = lambda i: [pieces[i]] + gathered[i]
        first = [[] for _ in range(1, ny)]
        for g in range(groups):
            held = jnp.where(stays, own[g], turned[g])
            blocks = [held] + [
                lax.ppermute(held, "row", [(r, (r + s) % rows) for r in range(rows)]) for s in range(1, rows)
            ]
            factors.append(arrange(place, blocks, nx, ny, depth))
            for t in range(1, ny):
                value = product([parts(0)], [[factors[g][t]]])[0][0]
                first[t - 1].append(lax.ppermute(value, "col", along_y(t)))
        near, sent = {}, {0: [jnp.concatenate(pair, axis=1) for pair in first]}

        def multiply(which):
            which = [i for i in which if i < n]
            if not which:
                return
            sets = [[group[t] for group in factors] for t in range(ny)]
            found = product([parts(i) for i in which], sets)
            for k, i in enumerate(which):
                near[i] = found[0][k]
                sent[i] = [lax.ppermute(found[t][k], "col", along_y(t)) for t in range(1, ny)]

        multiply(WORK[-2])
        near[0] = product([parts(0)], [[group[0] for group in factors]])[0][0]
        multiply(WORK[-1])
        starts = [unit * sum(SHARES[:i]) for i in range(n)]
        result = jnp.zeros((panels.shape[0], width), jnp.float32)
        total, summed, done, paired, crossed = {}, {}, {}, {}, {}
        for i in range(n + LAG + 2):
            multiply(WORK.get(i, ()))
            k = i - LAG
            if i < n and 0 <= k and SHARES[i] == SHARES[k]:
                total[i], done[k], give = combine(flag, [near[i], *sent[i]], [summed[k], crossed[k]])
                paired[i] = (lax.ppermute(give, "layer", pairs),) * 2
            else:
                paired[i] = [None, None]
                if i < n:
                    total[i] = combine(flag, [near[i], *sent[i]])[0]
                    paired[i][0] = lax.ppermute(total[i], "layer", pairs[0::3])
                if 0 <= k < n:
                    done[k] = combine(flag, [summed[k], crossed[k]])[0]
                    paired[i][1] = lax.ppermute(done[k], "layer", pairs[1:3])
            for late in LATE.get(i, ()):
                if late < n:
                    gather(late)
            k = i - 1
            if 0 <= k < n:
                summed[k] = combine(flag, [total[k], paired[k][0]])[0]
                crossed[k] = lax.ppermute(summed[k], "layer", across)
            k = i - LAG - 1
            if 0 <= k < n:
                value = jnp.where(end, paired[k + LAG][1], done[k])
                result = lax.dynamic_update_slice(result, value, (starts[k], 0))
        return result

    in_specs = (P("row", ("layer", "col")), P(("layer", "row"), "col"))
    out_specs = P("row", "col")
    step = jax.shard_map(body, mesh=mesh, in_specs=in_specs, out_specs=out_specs, check_vma=False)

    def traced(panels, eigvecs):
        jax.eval_shape(step, panels, eigvecs)
        return step(panels, eigvecs)

    return traced
```

```python
import jax
import jax.numpy as jnp
from jax import lax
from jax.experimental import pallas as pl
from jax.experimental.pallas import tpu as pltpu
from jax.sharding import PartitionSpec as P


SHARES = (6, 6, 6, 6, 6, 6, 6, 6, 6, 6, 4)
LAG = 3
EARLY = 5
LATE = {0: (5, 6), 1: (7, 8), 2: (9, 10)}
WORK = {-2: (1,), -1: (2,), 1: (3,), 2: (4,), 3: (5,), 4: (6,), 5: (7,), 6: (8,), 7: (9,), 8: (10,)}
VMEM = 12 * 2**20


def side(count):
    return max(i for i in range(1, count + 1) if i * i <= count and count % i == 0)


def halves(value):
    high = value.astype(jnp.bfloat16)
    return high, (value - high.astype(jnp.float32)).astype(jnp.bfloat16)


def product_kernel(pieces, nx, sets, groups, *refs):
    parts, factors = refs[:pieces * nx], refs[pieces * nx:pieces * nx + 2 * nx * sets * groups]
    outs = refs[len(parts) + len(factors):]
    terms = [halves(part[...]) for part in parts]
    for f in range(sets):
        for g in range(groups):
            chosen = factors[2 * nx * (f * groups + g):]
            totals = [None] * pieces
            for s in range(nx):
                high, low = chosen[2 * s][...], chosen[2 * s + 1][...]
                for which, b in ((1, high), (0, low), (0, high)):
                    for i in range(pieces):
                        term = jnp.dot(terms[i * nx + s][which], b, preferred_element_type=jnp.float32)
                        totals[i] = term if totals[i] is None else totals[i] + term
            for i in range(pieces):
                out = outs[f * pieces + i]
                width = out.shape[1] // groups
                out[:, g * width:(g + 1) * width] = totals[i]


def product(pieces, sets):
    nx, groups = len(pieces[0]), len(sets[0])
    width = sets[0][0][0].shape[1] * groups
    whole = lambda value: pl.BlockSpec(value.shape, lambda i: (0, 0))
    flat = [part for piece in pieces for part in piece] + [term for each in sets for group in each for term in group]
    results = [pltpu.VMEM((piece[0].shape[0], width), jnp.float32) for _ in sets for piece in pieces]
    flops = sum(6 * part.size * width * len(sets) for piece in pieces for part in piece)
    found = pl.pallas_call(
        lambda *refs: product_kernel(len(pieces), nx, len(sets), groups, *refs),
        grid=(1,),
        out_shape=results,
        in_specs=[whole(value) for value in flat],
        out_specs=[whole(result) for result in results],
        compiler_params=pltpu.CompilerParams(vmem_limit_bytes=VMEM),
        cost_estimate=pl.CostEstimate(flops=flops, bytes_accessed=flops // 3072, transcendentals=0),
        name="product",
    )(*flat)
    return [found[f * len(pieces):(f + 1) * len(pieces)] for f in range(len(sets))]


def arrange_kernel(nx, ny, depth, place, *refs):
    row, y, x = place[0], place[1], place[2]
    rows = len(refs) - 2 * nx * ny
    q = rows // ny
    for t in range(ny):
        for s in range(nx):
            value = None
            for back in range(rows):
                count = refs[back].shape[0] // depth
                index = (row - back + rows) % rows
                for c in range(count):
                    here = (index // q == (y + t) % ny) & ((index % q) * count + c == (x - s + nx) % nx)
                    chunk = refs[back][c * depth:(c + 1) * depth, :]
                    value = chunk if value is None else jnp.where(here, chunk, value)
            at = rows + 2 * (t * nx + s)
            refs[at][...], refs[at + 1][...] = halves(value)


def arrange(place, blocks, nx, ny, depth):
    width = blocks[0].shape[1]
    whole = lambda value: pl.BlockSpec(value.shape, lambda i: (0, 0))
    results = [pltpu.VMEM((depth, width), jnp.bfloat16)] * (2 * nx * ny)
    found = pl.pallas_call(
        lambda *refs: arrange_kernel(nx, ny, depth, *refs),
        grid=(1,),
        out_shape=results,
        in_specs=[pl.BlockSpec(memory_space=pltpu.SMEM)] + [whole(block) for block in blocks],
        out_specs=[whole(result) for result in results],
        compiler_params=pltpu.CompilerParams(vmem_limit_bytes=VMEM),
        cost_estimate=pl.CostEstimate(flops=blocks[0].size * 64, bytes_accessed=blocks[0].size * 16, transcendentals=0),
        name="arrange",
    )(place, *blocks)
    return [found[2 * nx * t:2 * nx * (t + 1)] for t in range(ny)]


def combine_kernel(counts, flag, *refs):
    ins, outs = refs[:sum(counts)], refs[sum(counts):]
    found, at = [], 0
    for count in counts:
        total = ins[at][...]
        for ref in ins[at + 1:at + count]:
            total = total + ref[...]
        found.append(total)
        at += count
    for total, out in zip(found, outs):
        out[...] = total
    if len(counts) > 1:
        outs[-1][...] = jnp.where(flag[0] == 1, found[0], found[1])


def combine(flag, *lists):
    shape = lists[0][0].shape
    flat = [value for values in lists for value in values]
    whole = pl.BlockSpec(shape, lambda i: (0, 0))
    results = [pltpu.VMEM(shape, jnp.float32)] * (len(lists) + (len(lists) > 1))
    return pl.pallas_call(
        lambda *refs: combine_kernel([len(values) for values in lists], *refs),
        grid=(1,),
        out_shape=results,
        in_specs=[pl.BlockSpec(memory_space=pltpu.SMEM)] + [whole] * len(flat),
        out_specs=[whole] * len(results),
        compiler_params=pltpu.CompilerParams(vmem_limit_bytes=VMEM),
        cost_estimate=pl.CostEstimate(flops=flat[0].size * 64, bytes_accessed=flat[0].size * 16, transcendentals=0),
        name="combine",
    )(flag, *flat)


def solution(mesh):
    layers, rows, cols = (mesh.shape[a] for a in ("layer", "row", "col"))
    nx = side(cols)
    ny = cols // nx
    if rows % ny or layers != 4:
        raise ValueError("mesh")
    q = rows // ny

    def along_x(shift):
        return [(y * nx + x, y * nx + (x + shift) % nx) for y in range(ny) for x in range(nx)]

    def along_y(shift):
        return [(y * nx + x, (y + shift) % ny * nx + x) for y in range(ny) for x in range(nx)]

    turn = [
        ((r * ny + y) * nx + x, ((y * q + r % q) * ny + r // q) * nx + x)
        for r in range(rows) for y in range(ny) for x in range(nx) if r // q != y
    ]
    pairs = [(0, 1), (1, 0), (2, 3), (3, 2)]
    across = [(1, 2), (2, 1)]

    def body(panels, eigvecs):
        layer, row = lax.axis_index("layer"), lax.axis_index("row")
        col = lax.axis_index("col")
        y, x = col // nx, col % nx
        end = (layer == 0) | (layer == layers - 1)
        depth = panels.shape[1]
        width = eigvecs.shape[1]
        groups = 2 if width % 256 == 0 else 1
        unit = panels.shape[0] // sum(SHARES)
        n = len(SHARES)
        pieces, at = [], 0
        for share in SHARES:
            pieces.append(panels[at:at + share * unit])
            at += share * unit

        own, source = [], eigvecs
        for g in range(groups):
            own.append(lax.optimization_barrier(source[:, g * width // groups:(g + 1) * width // groups]))
            if g + 1 < groups:
                source, own[g] = lax.optimization_barrier((source, own[g]))
        stays = row // q == y
        turned = [lax.ppermute(own[g], ("row", "col"), turn) for g in range(groups)]
        gathered = {}
        flag = end.astype(jnp.int32).reshape(1)

        def gather(i):
            gathered[i] = [lax.ppermute(pieces[i], "col", along_x(s)) for s in range(1, nx)]

        for i in range(EARLY):
            gather(i)

        place = jnp.stack([row, y, x])
        factors = []
        parts = lambda i: [pieces[i]] + gathered[i]
        first = [[] for _ in range(1, ny)]
        for g in range(groups):
            held = jnp.where(stays, own[g], turned[g])
            blocks = [held] + [
                lax.ppermute(held, "row", [(r, (r + s) % rows) for r in range(rows)]) for s in range(1, rows)
            ]
            factors.append(arrange(place, blocks, nx, ny, depth))
            for t in range(1, ny):
                value = product([parts(0)], [[factors[g][t]]])[0][0]
                first[t - 1].append(lax.ppermute(value, "col", along_y(t)))
        near, sent = {}, {0: [jnp.concatenate(pair, axis=1) for pair in first]}

        def multiply(which):
            which = [i for i in which if i < n]
            if not which:
                return
            sets = [[group[t] for group in factors] for t in range(ny)]
            found = product([parts(i) for i in which], sets)
            for k, i in enumerate(which):
                near[i] = found[0][k]
                sent[i] = [lax.ppermute(found[t][k], "col", along_y(t)) for t in range(1, ny)]

        multiply(WORK[-2])
        near[0] = product([parts(0)], [[group[0] for group in factors]])[0][0]
        multiply(WORK[-1])
        starts = [unit * sum(SHARES[:i]) for i in range(n)]
        result = jnp.zeros((panels.shape[0], width), jnp.float32)
        total, summed, done, paired, crossed = {}, {}, {}, {}, {}
        for i in range(n + LAG + 2):
            multiply(WORK.get(i, ()))
            k = i - LAG
            if i < n and 0 <= k and SHARES[i] == SHARES[k]:
                total[i], done[k], give = combine(flag, [near[i], *sent[i]], [summed[k], crossed[k]])
                paired[i] = (lax.ppermute(give, "layer", pairs),) * 2
            else:
                paired[i] = [None, None]
                if i < n:
                    total[i] = combine(flag, [near[i], *sent[i]])[0]
                    paired[i][0] = lax.ppermute(total[i], "layer", pairs[0::3])
                if 0 <= k < n:
                    done[k] = combine(flag, [summed[k], crossed[k]])[0]
                    paired[i][1] = lax.ppermute(done[k], "layer", pairs[1:3])
            for late in LATE.get(i, ()):
                if late < n:
                    gather(late)
            k = i - 1
            if 0 <= k < n:
                summed[k] = combine(flag, [total[k], paired[k][0]])[0]
                crossed[k] = lax.ppermute(summed[k], "layer", across)
            k = i - LAG - 1
            if 0 <= k < n:
                value = jnp.where(end, paired[k + LAG][1], done[k])
                result = lax.dynamic_update_slice(result, value, (starts[k], 0))
        return result

    in_specs = (P("row", ("layer", "col")), P(("layer", "row"), "col"))
    out_specs = P("row", "col")
    step = jax.shard_map(body, mesh=mesh, in_specs=in_specs, out_specs=out_specs, check_vma=False)

    def traced(panels, eigvecs):
        jax.eval_shape(step, panels, eigvecs)
        return step(panels, eigvecs)

    return traced
```
